32 devices in a mesh: ens: 4 (over y, x), slab: 8 (over z, core).
Axes of the slice: x: 2, y: 2, z: 4, core: 2. Of those that a mesh axis runs over, the one named last changes fastest.
Arguments:
- density0: float32 [192, 1024], P('slab'), may hold values from 0.5 to 1.5
- relax_rate: float32 [192, 1024], P('slab'), may hold values from 0.6 to 1.8
- perturbation: int32 [4, 192, 1024], P('ens', 'slab'), may hold values from -3 to 3
Outputs:
- lifted: float32 [4, 9, 192, 1024], P('ens', None, 'slab')
- projected: float32 [192, 1024], P('slab')
The draws below stay inside these ranges and needn't reach their ends.
All inputs are finite; a program needn't handle non-finite values.
Results may differ from the reference program's by a relative error of at most 0.0002.
Values sent between devices are 32-bit elements; how exact they have to be, the bound alone decides.
A program may use at most 64 MiB of HBM per device.

```python
import jax
import jax.numpy as jnp
from jax import lax

NC = 1024
MICRO_SPELLS = 3
STEPS = 8
MEMBERS = 4
NR = 192


def draw_density0(key, part):
    row_index = jnp.arange(NR, dtype=jnp.float32)
    row_ramp = 1.0 + 2.0 * row_index / max(NR - 1, 1)
    roughness = jax.random.truncated_normal(key, -4.0, 4.0, (NR, NC), jnp.float32)
    return 1.0 + 0.03 * row_ramp[:, None] * roughness


def set_ends(result, own_key, smallest, top_value):
    spot = [jax.random.randint(jax.random.fold_in(own_key, axis), (), 0, length) for axis, length in enumerate(result.shape)]
    longest = result.shape.index(max(result.shape))
    neighbour = spot[:longest] + [(spot[longest] + 1) % result.shape[longest]] + spot[longest + 1:]
    return result.at[tuple(spot)].set(smallest).at[tuple(neighbour)].set(top_value)


def levels(own_key, shape, shards, smallest, top_value):
    factor_of = 1.0
    for axis_at, shards_of in shards:
        steps = jax.random.uniform(jax.random.fold_in(jax.random.fold_in(own_key, 6), axis_at), (shards_of,), jnp.float32, smallest / len(shards), top_value / len(shards))
        factor_of = factor_of * jnp.repeat(jnp.exp(steps), shape[axis_at] // shards_of).reshape((-1,) + (1,) * (len(shape) - 1 - axis_at))
    return factor_of


def setup_inputs(seed: int = 0) -> dict:
    key_of = jax.random.split(jax.random.key(seed), 4)
    density0 = draw_density0(jax.random.fold_in(key_of[3], 71), 0)
    relax_rate = jnp.clip(0.6 + 1.1999999 * jax.random.uniform(key_of[1], (NR, NC), jnp.float32) ** levels(key_of[1], (NR, NC), ((0, 8),), -0.2, 0.2), 0.6, 1.8)
    perturbation = set_ends(jax.random.randint(key_of[2], (MEMBERS, NR, NC), -3, 4), jax.random.fold_in(key_of[2], 1), -3, 3).astype(jnp.int32)
    return {"density0": density0, "relax_rate": relax_rate, "perturbation": perturbation}


vertical_lattice_offsets = (0, 0, 1, 0, -1, 1, 1, -1, -1)
col_moves = (0, 1, 0, -1, 0, 1, -1, -1, 1)
lattice_weights = (4.0 / 9.0, 1.0 / 9.0, 1.0 / 9.0, 1.0 / 9.0, 1.0 / 9.0, 1.0 / 36.0, 1.0 / 36.0, 1.0 / 36.0, 1.0 / 36.0)
shift_amp = 0.08
step_cap = 0.25

def collide(distrib, relax_rate):
    density = distrib[..., 0, :, :]
    for direction in range(1, 9):
        density = density + distrib[..., direction, :, :]
    mom_row = distrib[..., 2, :, :] + distrib[..., 5, :, :] + distrib[..., 6, :, :] - (distrib[..., 4, :, :] + distrib[..., 7, :, :] + distrib[..., 8, :, :])
    mom_col = distrib[..., 1, :, :] + distrib[..., 5, :, :] + distrib[..., 8, :, :] - (distrib[..., 3, :, :] + distrib[..., 6, :, :] + distrib[..., 7, :, :])
    vel_row = mom_row / density
    vel_col = mom_col / density
    speed_sq = vel_row * vel_row + vel_col * vel_col
    relaxed = []
    for direction in range(9):
        along = vertical_lattice_offsets[direction] * vel_row + col_moves[direction] * vel_col
        equilib = lattice_weights[direction] * density * (1.0 + 3.0 * along + 4.5 * along * along - 1.5 * speed_sq)
        current = distrib[..., direction, :, :]
        relaxed.append(current - relax_rate * (current - equilib))
    return jnp.stack(relaxed, axis=-3)

def stream_full(relaxed):
    moved = [jnp.roll(relaxed[..., direction, :, :], (vertical_lattice_offsets[direction], col_moves[direction]), axis=(-2, -1)) for direction in range(9)]
    return jnp.stack(moved, axis=-3)

def reference(density0, relax_rate, perturbation):
    starts = density0[None] + shift_amp * perturbation.astype(jnp.float32)

    def advance_replica(start):
        distrib = jnp.stack([weight * start for weight in lattice_weights], axis=0)
        samples = []
        for spell_ordinal in range(MICRO_SPELLS):
            for step_index in range(STEPS):
                distrib = stream_full(collide(distrib, relax_rate))
            samples.append(lax.optimization_barrier(jnp.sum(distrib, axis=0)))
        return (distrib, jnp.stack(samples))
    finals, samples = lax.map(advance_replica, starts)
    totals = lax.optimization_barrier(jnp.sum(samples, axis=0))
    ensemble_mean = totals / MEMBERS
    first = ensemble_mean[0]
    middle = ensemble_mean[1]
    last = ensemble_mean[2]
    change = last - first
    fitted_slope = (first + middle + last) / 3.0 + 0.5 * change
    mean_square = jnp.sum(change * change) / (NR * NC)
    projected = fitted_slope + step_cap * change / jnp.sqrt(mean_square + 1e-06)
    lifted = finals * (projected[None] / samples[:, 2])[:, None]
    return (lifted, projected)
```

```python
import functools

import jax
import jax.numpy as jnp
from jax import lax
from jax.experimental import pallas as pl
from jax.experimental.pallas import tpu as pltpu
from jax.sharding import PartitionSpec as P

MICRO_SPELLS = 3
STEPS = 8
TOTAL = MICRO_SPELLS * STEPS
LANES = 128
TILE = 8
WIDE = 4

row_moves = (0, 0, 1, 0, -1, 1, 1, -1, -1)
col_moves = (0, 1, 0, -1, 0, 1, -1, -1, 1)
mirrored = (0, 1, 4, 3, 2, 8, 7, 6, 5)
lattice_weights = (4.0 / 9.0,) + (1.0 / 9.0,) * 4 + (1.0 / 36.0,) * 4
shift_amp = 0.08
step_cap = 0.25
MESH = pl.DeviceIdType.MESH
OWN, NEAR, FAR = 0, 1, 2
DUMMY = MICRO_SPELLS


def collide(f, keep, third, ninth):
    plus = f[1] + (f[5] + f[8])
    minus = f[3] + (f[6] + f[7])
    density = (f[0] + (f[2] + f[4])) + (plus + minus)
    mom_col = plus - minus
    mom_row = (f[2] - f[4]) + ((f[5] + f[6]) - (f[7] + f[8]))
    inverse = 1.5 / density
    vel_row = mom_row * inverse
    vel_col = mom_col * inverse
    third_row = third * mom_row
    third_col = third * mom_col
    half_rr = third_row * vel_row
    half_cc = third_col * vel_col
    quarter_rc = (third_row * vel_col) * 0.5
    squares = half_rr + half_cc
    base = ninth * density - squares * (1.0 / 3.0)
    even_col = base + half_cc
    even_row = base + half_rr
    corner = 0.25 * (base + squares)
    even_57 = corner + quarter_rc
    even_68 = corner - quarter_rc
    odd_57 = 0.25 * (third_row + third_col)
    odd_68 = 0.25 * (third_row - third_col)
    out = (
        keep * f[0] + 4.0 * base,
        keep * f[1] + (even_col + third_col),
        keep * f[2] + (even_row + third_row),
        keep * f[3] + (even_col - third_col),
        keep * f[4] + (even_row - third_row),
        keep * f[5] + (even_57 + odd_57),
        keep * f[6] + (even_68 + odd_68),
        keep * f[7] + (even_57 - odd_57),
        keep * f[8] + (even_68 - odd_68),
    )
    return out, density


def kernel(
    ens,
    slabs,
    density_hbm,
    relax_hbm,
    pert_hbm,
    finals,
    scale_out,
    projected_out,
    density_in,
    pert_in,
    raws,
    even,
    odd,
    coef,
    gathered,
    change_at,
    fitted_at,
    squares,
    in_sem,
    halo_send,
    halo_recv,
    ens_send,
    ens_recv,
    sq_send,
    sq_recv,
):
    height, width = density_in.shape
    blocks = width // LANES
    chunks = height // TILE
    wide = WIDE if blocks % WIDE == 0 else 1
    me_e = lax.axis_index("ens")
    me_s = lax.axis_index("slab")
    flipped = lax.rem(me_s, 2)

    barrier = pltpu.get_barrier_semaphore()
    for k in range(1, ens):
        pl.semaphore_signal(
            barrier, inc=1, device_id={"ens": lax.rem(me_e + k, ens)}, device_id_type=MESH
        )
    for k in range(1, slabs):
        pl.semaphore_signal(
            barrier, inc=1, device_id={"slab": lax.rem(me_s + k, slabs)}, device_id_type=MESH
        )

    loads = [
        pltpu.make_async_copy(density_hbm, density_in, in_sem.at[0]),
        pltpu.make_async_copy(pert_hbm.at[0], pert_in, in_sem.at[1]),
        pltpu.make_async_copy(relax_hbm, raws.at[OWN, 1], in_sem.at[2]),
    ]
    for copy in loads:
        copy.start()

    lane = lax.broadcasted_iota(jnp.int32, (TILE, LANES), 1)
    sublane = lax.broadcasted_iota(jnp.int32, (TILE, LANES), 0)
    order = jnp.where(flipped == 1, TILE - 1 - sublane, sublane)
    edges = {1: lane == 0, -1: lane == LANES - 1}
    bodies = {1: lane != 0, -1: lane != LANES - 1}

    def flip(x):
        return jnp.take_along_axis(x, order, axis=0, mode="promise_in_bounds")

    def natural(c):
        return pl.multiple_of(TILE * jnp.where(flipped == 1, chunks - 1 - c, c), TILE)

    def moved_store(ref, at, first, x, move):
        count = x.shape[0]
        over = lambda mask, n: jnp.broadcast_to(mask[None], (n, TILE, LANES))
        turned = pltpu.roll(x, 1 if move == 1 else LANES - 1, 2)
        pltpu.store(
            ref.at[pl.ds(first, count), at, :], turned, mask=over(bodies[move], count)
        )
        edge = edges[move]
        low = first + move
        if low < 0:
            pltpu.store(ref.at[pl.ds(blocks - 1, 1), at, :], turned[:1], mask=over(edge, 1))
            turned, low, count = turned[1:], 0, count - 1
        elif low + count > blocks:
            pltpu.store(ref.at[pl.ds(0, 1), at, :], turned[count - 1 :], mask=over(edge, 1))
            turned, count = turned[: count - 1], count - 1
        if count:
            pltpu.store(ref.at[pl.ds(low, count), at, :], turned, mask=over(edge, count))

    def fill(place, offset):
        def body(c, carry):
            at = pl.ds(offset + c * TILE, TILE)
            rows = pl.ds(natural(c), TILE)
            for b in range(blocks):
                cols = slice(b * LANES, (b + 1) * LANES)
                rate = flip(raws[place, 1, rows, cols])
                fresh = flip(raws[place, 0, rows, cols])
                coef[0, b, at, :] = 1.0 - rate
                coef[1, b, at, :] = rate * (1.0 / 3.0)
                coef[2, b, at, :] = rate * (1.0 / 9.0)
                for weight, members in (
                    (lattice_weights[0], (0,)),
                    (lattice_weights[1], (1, 2, 3, 4)),
                    (lattice_weights[5], (5, 6, 7, 8)),
                ):
                    part = weight * fresh
                    for i in members:
                        if col_moves[i] == 0:
                            odd[i, b, at, :] = part
                        else:
                            moved_store(odd.at[i], at, b, part[None], col_moves[i])
            return carry

        lax.fori_loop(0, chunks, body, 0)

    front = height

    def group(k, low, slot=None):
        source, dest = (odd, even) if k % 2 == 0 else (even, odd)
        at = front + low
        rows = pl.ds(at, TILE)
        for first in range(0, blocks, wide):
            cols = pl.ds(first, wide)
            f = [source[i, cols, pl.ds(at - row_moves[i], TILE), :] for i in range(9)]
            out, density = collide(f, *(coef[n, cols, rows, :] for n in range(3)))
            if slot is not None:
                gathered[slot, me_e, cols, rows, :] = density
            for i in range(9):
                if col_moves[i] == 0:
                    dest[i, cols, rows, :] = out[i]
                else:
                    moved_store(dest.at[i], rows, first, out[i], col_moves[i])

    for copy in loads:
        copy.wait()
    for c in range(chunks):
        rows = slice(c * TILE, (c + 1) * TILE)
        raws[OWN, 0, rows, :] = density_in[rows, :] + shift_amp * pert_in[rows, :].astype(
            jnp.float32
        )
    fill(OWN, front)

    def triangle(k):
        low, high = k - 1, height + 1 - k
        for first in range(low, high, TILE):
            group(k, min(first, high - TILE), 0 if k == STEPS + 1 else None)

    triangle(2)
    pl.semaphore_wait(barrier, ens + slabs - 2)
    near_to = me_s + 1 - 2 * flipped
    far_to = lax.rem(me_s + slabs - 1 + 2 * flipped, slabs)
    halos = {}
    for place, target in ((FAR, far_to), (NEAR, near_to)):
        halos[place] = [
            pltpu.make_async_remote_copy(
                src_ref=raws.at[OWN, n],
                dst_ref=raws.at[place, n],
                send_sem=halo_send.at[place - 1, n],
                recv_sem=halo_recv.at[place - 1, n],
                device_id={"slab": target},
                device_id_type=MESH,
            )
            for n in (1, 0)
        ]
        for copy in halos[place]:
            copy.start()
    for k in range(3, STEPS + 2):
        triangle(k)

    for copy in halos[NEAR]:
        copy.wait_recv()
    fill(NEAR, front + height)

    def lean(t, carry):
        for n in range(4):
            k = 2 + 4 * t + n
            for j in range(chunks - 1, -1, -1):
                slot = jnp.where(t == 1, 0, DUMMY) if n == 3 else None
                group(n % 2, height + 1 - k + TILE * j, slot)
        return carry

    lax.fori_loop(0, 2, lean, 0)
    for k in range(STEPS + 2, TOTAL + 1):
        count = 2 * height + 2 - 2 * k
        for j in range((count + TILE - 1) // TILE - 1, -1, -1):
            group(k, k - 1 + TILE * j, 1 if k == 2 * STEPS + 1 else None)

    for copy in halos[FAR]:
        copy.wait_recv()
    fill(FAR, front - height)

    def strips(t, carry):
        for n in range(4):
            k = 2 + 4 * t + n
            for j in range(1, chunks + 1):
                slot = None
                if n == 3:
                    slot = jnp.where(t == 1, 0, jnp.where(t == 3, 1, DUMMY))
                group(n % 2, k - 1 - TILE * j, slot)
        return carry

    def send_spell(spell):
        copies = []
        own = pl.ds(front, height)
        for k in range(1, ens):
            copies.append(
                pltpu.make_async_remote_copy(
                    src_ref=gathered.at[spell, me_e, :, own],
                    dst_ref=gathered.at[spell, me_e, :, own],
                    send_sem=ens_send.at[spell, k - 1],
                    recv_sem=ens_recv.at[spell, k - 1],
                    device_id={"ens": lax.rem(me_e + k, ens)},
                    device_id_type=MESH,
                )
            )
        for copy in copies:
            copy.start()
        return copies

    lax.fori_loop(0, 2, strips, 0)
    sent = [send_spell(0)]
    lax.fori_loop(2, 4, strips, 0)
    sent.append(send_spell(1))
    for k in range(2 * STEPS + 2, TOTAL + 1):
        for j in range(1, chunks + 1):
            group(k, k - 1 - TILE * j)

    last = even if TOTAL % 2 == 0 else odd

    def settle(c, carry):
        at = front + c * TILE
        for b in range(blocks):
            total = last[0, b, pl.ds(at, TILE), :]
            for i in range(1, 9):
                total = total + last[i, b, pl.ds(at - row_moves[i], TILE), :]
            gathered[MICRO_SPELLS - 1, me_e, b, pl.ds(at, TILE), :] = total
        return carry

    lax.fori_loop(0, chunks, settle, 0)
    sent.append(send_spell(MICRO_SPELLS - 1))

    def put_finals(c, carry):
        at = front + c * TILE
        rows = pl.ds(natural(c), TILE)
        for i in range(9):
            to = jnp.where(flipped == 1, mirrored[i], i)
            for b in range(blocks):
                cols = slice(b * LANES, (b + 1) * LANES)
                finals[to, rows, cols] = flip(last[i, b, pl.ds(at - row_moves[i], TILE), :])
        return carry

    lax.fori_loop(0, chunks, put_finals, 0)

    for copies in sent:
        for copy in copies:
            copy.wait_recv()

    def mean(spell, at):
        total = gathered[spell, 0, :, at, :]
        for member in range(1, ens):
            total = total + gathered[spell, member, :, at, :]
        return total * (1.0 / ens)

    def fit(c, acc):
        at = pl.ds(front + c * TILE, TILE)
        to = pl.ds(pl.multiple_of(c * TILE, TILE), TILE)
        first, middle, final = (mean(spell, at) for spell in range(MICRO_SPELLS))
        change = final - first
        change_at[:, to, :] = change
        fitted_at[:, to, :] = (first + middle + final) * (1.0 / 3.0) + 0.5 * change
        return acc + jnp.sum(change * change, axis=0)

    acc = lax.fori_loop(0, chunks, fit, jnp.zeros((TILE, LANES), jnp.float32))
    squares[me_s] = acc
    copies = []
    for k in range(1, slabs):
        copies.append(
            pltpu.make_async_remote_copy(
                src_ref=squares.at[me_s],
                dst_ref=squares.at[me_s],
                send_sem=sq_send.at[k - 1],
                recv_sem=sq_recv.at[k - 1],
                device_id={"slab": lax.rem(me_s + k, slabs)},
                device_id_type=MESH,
            )
        )
    for copy in copies:
        copy.start()
    for copy in copies:
        copy.wait_recv()
    total = jnp.sum(jnp.sum(squares[...], axis=0), axis=(0, 1), keepdims=True)
    mean_square = total * (1.0 / (height * width * slabs))
    gain = step_cap / jnp.sqrt(mean_square + 1e-06)

    def project(c, carry):
        at = pl.ds(front + c * TILE, TILE)
        here = pl.ds(pl.multiple_of(c * TILE, TILE), TILE)
        rows = pl.ds(natural(c), TILE)
        for b in range(blocks):
            cols = slice(b * LANES, (b + 1) * LANES)
            projected = fitted_at[b, here, :] + gain * change_at[b, here, :]
            projected_out[rows, cols] = flip(projected)
            scale_out[rows, cols] = flip(
                projected / gathered[MICRO_SPELLS - 1, me_e, b, at, :]
            )
        return carry

    lax.fori_loop(0, chunks, project, 0)

    for group_of in [halos[NEAR], halos[FAR], copies] + sent:
        for copy in group_of:
            copy.wait_send()


def on_device(density0, relax_rate, perturbation):
    height, width = density0.shape
    ens, slabs = lax.axis_size("ens"), lax.axis_size("slab")
    assert perturbation.shape[0] == 1 and width % LANES == 0
    assert height == TOTAL and height % TILE == 0 and slabs % 2 == 0
    blocks = width // LANES
    rows = 3 * height
    f32 = jnp.float32
    field = jax.ShapeDtypeStruct((height, width), f32)
    vmem = pl.BlockSpec(memory_space=pltpu.VMEM)
    dma = pltpu.SemaphoreType.DMA
    finals, scale, projected = pl.pallas_call(
        functools.partial(kernel, ens, slabs),
        out_shape=(
            jax.ShapeDtypeStruct((9, height, width), f32),
            field,
            field,
        ),
        in_specs=[pl.BlockSpec(memory_space=pltpu.HBM)] * 3,
        out_specs=[vmem] * 3,
        scratch_shapes=[
            pltpu.VMEM((height, width), f32),
            pltpu.VMEM((height, width), jnp.int32),
            pltpu.VMEM((3, 2, height, width), f32),
            pltpu.VMEM((9, blocks, rows, LANES), f32),
            pltpu.VMEM((9, blocks, rows, LANES), f32),
            pltpu.VMEM((3, blocks, rows, LANES), f32),
            pltpu.VMEM((MICRO_SPELLS + 1, ens, blocks, rows, LANES), f32),
            pltpu.VMEM((blocks, height, LANES), f32),
            pltpu.VMEM((blocks, height, LANES), f32),
            pltpu.VMEM((slabs, TILE, LANES), f32),
            dma((3,)),
            dma((2, 2)),
            dma((2, 2)),
            dma((MICRO_SPELLS, ens - 1)),
            dma((MICRO_SPELLS, ens - 1)),
            dma((slabs - 1,)),
            dma((slabs - 1,)),
        ],
        compiler_params=pltpu.CompilerParams(
            collective_id=0, has_side_effects=True, vmem_limit_bytes=48 << 20
        ),
    )(density0, relax_rate, perturbation)
    lifted = finals * scale[None]
    return (lifted[None], projected)


def solution(mesh):
    in_specs = (P("slab", None), P("slab", None), P("ens", "slab", None))
    out_specs = (P("ens", None, "slab", None), P("slab", None))
    return jax.shard_map(
        on_device, mesh=mesh, in_specs=in_specs, out_specs=out_specs, check_vma=False
    )
```

```python
import functools

import jax
import jax.numpy as jnp
from jax import lax
from jax.experimental import pallas as pl
from jax.experimental.pallas import tpu as pltpu
from jax.sharding import PartitionSpec as P

MICRO_SPELLS = 3
STEPS = 8
TOTAL = MICRO_SPELLS * STEPS
LANES = 128
TILE = 8
WIDE = 4

row_moves = (0, 0, 1, 0, -1, 1, 1, -1, -1)
col_moves = (0, 1, 0, -1, 0, 1, -1, -1, 1)
mirrored = (0, 1, 4, 3, 2, 8, 7, 6, 5)
lattice_weights = (4.0 / 9.0,) + (1.0 / 9.0,) * 4 + (1.0 / 36.0,) * 4
shift_amp = 0.08
step_cap = 0.25
MESH = pl.DeviceIdType.MESH
OWN, NEAR, FAR = 0, 1, 2
DUMMY = MICRO_SPELLS - 1
PIECES = 5


def collide(f, keep, third, ninth):
    plus = f[1] + (f[5] + f[8])
    minus = f[3] + (f[6] + f[7])
    density = (f[0] + (f[2] + f[4])) + (plus + minus)
    mom_col = plus - minus
    mom_row = (f[2] - f[4]) + ((f[5] + f[6]) - (f[7] + f[8]))
    inverse = 1.5 / density
    vel_row = mom_row * inverse
    vel_col = mom_col * inverse
    third_row = third * mom_row
    third_col = third * mom_col
    half_rr = third_row * vel_row
    half_cc = third_col * vel_col
    quarter_rc = (third_row * vel_col) * 0.5
    squares = half_rr + half_cc
    base = ninth * density - squares * (1.0 / 3.0)
    even_col = base + half_cc
    even_row = base + half_rr
    corner = 0.25 * (base + squares)
    even_57 = corner + quarter_rc
    even_68 = corner - quarter_rc
    odd_57 = 0.25 * (third_row + third_col)
    odd_68 = 0.25 * (third_row - third_col)
    out = (
        keep * f[0] + 4.0 * base,
        keep * f[1] + (even_col + third_col),
        keep * f[2] + (even_row + third_row),
        keep * f[3] + (even_col - third_col),
        keep * f[4] + (even_row - third_row),
        keep * f[5] + (even_57 + odd_57),
        keep * f[6] + (even_68 + odd_68),
        keep * f[7] + (even_57 - odd_57),
        keep * f[8] + (even_68 - odd_68),
    )
    return out, density


def kernel(
    ens,
    slabs,
    density_hbm,
    relax_hbm,
    pert_hbm,
    finals,
    scale_out,
    projected_out,
    density_in,
    pert_in,
    raws,
    even,
    odd,
    coef,
    gathered,
    partial,
    received,
    change_at,
    fitted_at,
    squares,
    in_sem,
    near_send,
    near_recv,
    far_send,
    far_recv,
    ens_send,
    ens_recv,
    pair_send,
    pair_recv,
    sq_send,
    sq_recv,
):
    height, width = density_in.shape
    blocks = width // LANES
    chunks = height // TILE
    wide = WIDE if blocks % WIDE == 0 else 1
    phases = ens.bit_length() - 1
    me_e = lax.axis_index("ens")
    me_s = lax.axis_index("slab")
    flipped = lax.rem(me_s, 2)

    barrier = pltpu.get_barrier_semaphore()
    for k in range(1, ens):
        pl.semaphore_signal(
            barrier, inc=1, device_id={"ens": lax.rem(me_e + k, ens)}, device_id_type=MESH
        )
    for k in range(1, slabs):
        pl.semaphore_signal(
            barrier, inc=1, device_id={"slab": lax.rem(me_s + k, slabs)}, device_id_type=MESH
        )

    loads = [
        pltpu.make_async_copy(density_hbm, density_in, in_sem.at[0]),
        pltpu.make_async_copy(pert_hbm.at[0], pert_in, in_sem.at[1]),
        pltpu.make_async_copy(relax_hbm, raws.at[OWN, 1], in_sem.at[2]),
    ]
    for copy in loads:
        copy.start()

    lane = lax.broadcasted_iota(jnp.int32, (TILE, LANES), 1)
    sublane = lax.broadcasted_iota(jnp.int32, (TILE, LANES), 0)
    order = jnp.where(flipped == 1, TILE - 1 - sublane, sublane)
    edges = {1: lane == 0, -1: lane == LANES - 1}
    bodies = {1: lane != 0, -1: lane != LANES - 1}

    def flip(x):
        return jnp.take_along_axis(x, order, axis=0, mode="promise_in_bounds")

    def natural(c):
        return pl.multiple_of(TILE * jnp.where(flipped == 1, chunks - 1 - c, c), TILE)

    def moved_store(ref, at, first, x, move):
        count = x.shape[0]
        over = lambda mask, n: jnp.broadcast_to(mask[None], (n, TILE, LANES))
        turned = pltpu.roll(x, 1 if move == 1 else LANES - 1, 2)
        pltpu.store(
            ref.at[pl.ds(first, count), at, :], turned, mask=over(bodies[move], count)
        )
        edge = edges[move]
        low = first + move
        if low < 0:
            pltpu.store(ref.at[pl.ds(blocks - 1, 1), at, :], turned[:1], mask=over(edge, 1))
            turned, low, count = turned[1:], 0, count - 1
        elif low + count > blocks:
            pltpu.store(ref.at[pl.ds(0, 1), at, :], turned[count - 1 :], mask=over(edge, 1))
            turned, count = turned[: count - 1], count - 1
        if count:
            pltpu.store(ref.at[pl.ds(low, count), at, :], turned, mask=over(edge, count))

    def fill(place, offset, which):
        for c in which:
            at = pl.ds(offset + c * TILE, TILE)
            rows = pl.ds(natural(c), TILE)
            for b in range(blocks):
                cols = slice(b * LANES, (b + 1) * LANES)
                rate = flip(raws[place, 1, rows, cols])
                fresh = flip(raws[place, 0, rows, cols])
                coef[0, b, at, :] = 1.0 - rate
                coef[1, b, at, :] = rate * (1.0 / 3.0)
                coef[2, b, at, :] = rate * (1.0 / 9.0)
                for weight, members in (
                    (lattice_weights[0], (0,)),
                    (lattice_weights[1], (1, 2, 3, 4)),
                    (lattice_weights[5], (5, 6, 7, 8)),
                ):
                    part = weight * fresh
                    for i in members:
                        if col_moves[i] == 0:
                            odd[i, b, at, :] = part
                        else:
                            moved_store(odd.at[i], at, b, part[None], col_moves[i])

    front = height

    def group(k, low, slot=None):
        source, dest = (odd, even) if k % 2 == 0 else (even, odd)
        at = front + low
        rows = pl.ds(at, TILE)
        for first in range(0, blocks, wide):
            cols = pl.ds(first, wide)
            f = [source[i, cols, pl.ds(at - row_moves[i], TILE), :] for i in range(9)]
            out, density = collide(f, *(coef[n, cols, rows, :] for n in range(3)))
            if slot is not None:
                gathered[slot, me_e, cols, rows, :] = density
            for i in range(9):
                if col_moves[i] == 0:
                    dest[i, cols, rows, :] = out[i]
                else:
                    moved_store(dest.at[i], rows, first, out[i], col_moves[i])

    for copy in loads:
        copy.wait()
    for c in range(chunks):
        rows = slice(c * TILE, (c + 1) * TILE)
        raws[OWN, 0, rows, :] = density_in[rows, :] + shift_amp * pert_in[rows, :].astype(
            jnp.float32
        )
    fill(OWN, front, range(chunks))

    def triangle(k):
        low, high = k - 1, height + 1 - k
        for first in range(low, high, TILE):
            group(k, min(first, high - TILE), 0 if k == STEPS + 1 else None)

    triangle(2)
    triangle(3)
    pl.semaphore_wait(barrier, ens + slabs - 2)
    near_to = me_s + 1 - 2 * flipped
    far_to = lax.rem(me_s + slabs - 1 + 2 * flipped, slabs)
    far = []
    for c in range(chunks):
        rows = pl.ds(natural(c), TILE)
        far.append(
            pltpu.make_async_remote_copy(
                src_ref=raws.at[OWN, :, rows],
                dst_ref=raws.at[FAR, :, rows],
                send_sem=far_send.at[c],
                recv_sem=far_recv.at[c],
                device_id={"slab": far_to},
                device_id_type=MESH,
            )
        )
    near = pltpu.make_async_remote_copy(
        src_ref=raws.at[OWN],
        dst_ref=raws.at[NEAR],
        send_sem=near_send,
        recv_sem=near_recv,
        device_id={"slab": near_to},
        device_id_type=MESH,
    )
    near.start()
    for copy in far:
        copy.start()
    for k in range(4, STEPS + 2):
        triangle(k)

    near.wait_recv()
    fill(NEAR, front + height, range(chunks))

    def lean(t, base):
        for n in range(4):
            for j in range(chunks):
                slot = jnp.where(t == 1, 0, DUMMY) if n == 3 else None
                group(n % 2, base + (TILE * j - n), slot)
        return base - 4

    sent = []

    def send(spell, low, high):
        own = pl.ds(front + low, high - low)
        piece = len(sent)
        copies = []
        for k in range(1, ens):
            copies.append(
                pltpu.make_async_remote_copy(
                    src_ref=gathered.at[spell, me_e, :, own],
                    dst_ref=gathered.at[spell, me_e, :, own],
                    send_sem=ens_send.at[piece, k - 1],
                    recv_sem=ens_recv.at[piece, k - 1],
                    device_id={"ens": lax.rem(me_e + k, ens)},
                    device_id_type=MESH,
                )
            )
        for copy in copies:
            copy.start()
        sent.append(copies)

    def near_side(k):
        count = 2 * height + 2 - 2 * k
        for j in range((count + TILE - 1) // TILE - 1, -1, -1):
            group(k, k - 1 + TILE * j, sample.get(k))

    def strip(m, k):
        if 2 <= k <= TOTAL:
            group(k, k - 1 - TILE * m, sample.get(k))

    def arrived(c):
        far[c].wait_recv()
        fill(FAR, front - height, (chunks - 1 - c,))

    def settle(b, c):
        at = front + c * TILE
        total = last[0, b, pl.ds(at, TILE), :]
        for i in range(1, 9):
            total = total + last[i, b, pl.ds(at - row_moves[i], TILE), :]
        return total

    cuts = [blocks * p // phases for p in range(phases + 1)]

    def pair(n, q, p):
        stride = 2 ** ((p + q) % phases)
        peer = me_e + stride - 2 * stride * lax.rem(me_e // stride, 2)
        part = pl.ds(cuts[p], cuts[p + 1] - cuts[p])
        return pltpu.make_async_remote_copy(
            src_ref=partial.at[n, q, part],
            dst_ref=received.at[n, q, part],
            send_sem=pair_send.at[n, q, p],
            recv_sem=pair_recv.at[n, q, p],
            device_id={"ens": peer},
            device_id_type=MESH,
        )

    pairs = [[[pair(n, q, p) for p in range(phases)] for q in range(phases)] for n in range(3)]

    def send_pairs(n, c):
        for b in range(blocks):
            partial[n, 0, b] = settle(b, c)
        for copy in pairs[n][0]:
            copy.start()

    last = even if TOTAL % 2 == 0 else odd
    sample = {STEPS + 1: 0, 2 * STEPS + 1: 1}
    lax.fori_loop(0, 2, lean, height - 1)
    send(0, STEPS, height)
    for k in range(STEPS + 2, STEPS + 5):
        near_side(k)
    arrived(0)
    for n in range(TOTAL + 10):
        if n == 7:
            send(1, 2 * STEPS, height)
            arrived(1)
        if n == 11:
            send(0, 0, STEPS)
            arrived(2)
        if n == 16:
            send(1, STEPS, 2 * STEPS)
        if n == 23:
            for b in range(blocks):
                partial[2, 0, b] = gathered[1, me_e, b, pl.ds(front, TILE), :]
            send_pairs(0, 2)
            for copy in pairs[2][0]:
                copy.start()
        if n == 30:
            send_pairs(1, 1)
        if STEPS + 5 + n <= TOTAL:
            near_side(STEPS + 5 + n)
        strip(1, n + 2)
        strip(2, n - 5)
        strip(3, n - 9)
    for b in range(blocks):
        gathered[MICRO_SPELLS - 1, me_e, b, pl.ds(front, TILE), :] = settle(b, 0)
    send(MICRO_SPELLS - 1, 0, TILE)

    def put_finals(c, carry):
        at = front + c * TILE
        rows = pl.ds(natural(c), TILE)
        for i in range(9):
            to = jnp.where(flipped == 1, mirrored[i], i)
            for b in range(blocks):
                cols = slice(b * LANES, (b + 1) * LANES)
                finals[to, rows, cols] = flip(last[i, b, pl.ds(at - row_moves[i], TILE), :])
        return carry

    lax.fori_loop(0, chunks, put_finals, 0)

    def direct(spell, b, low, count):
        at = pl.ds(front + low, count)
        total = gathered[spell, 0, b, at, :]
        for member in range(1, ens):
            total = total + gathered[spell, member, b, at, :]
        return total * (1.0 / ens)

    def paired(n, b):
        return (partial[n, phases - 1, b] + received[n, phases - 1, b]) * (1.0 / ens)

    def pass_on(n):
        for q in range(phases - 1):
            for p in range(phases):
                part = slice(cuts[p], cuts[p + 1])
                pairs[n][q][p].wait_recv()
                partial[n, q + 1, part] = partial[n, q, part] + received[n, q, part]
                pairs[n][q + 1][p].start()

    def early(b, carry):
        change_at[b] = direct(0, b, 0, height)
        fitted_at[b, pl.ds(TILE, height - TILE), :] = direct(1, b, TILE, height - TILE)
        return carry

    pass_on(0)
    for copies in sent[:-1]:
        for copy in copies:
            copy.wait_recv()
    lax.fori_loop(0, blocks, early, 0)
    pass_on(2)
    pass_on(1)
    for copy in pairs[2][phases - 1]:
        copy.wait_recv()
    for b in range(blocks):
        fitted_at[b, 0:TILE] = paired(2, b)
    for b in range(blocks):
        first = change_at[b]
        fitted_at[b] = (first + fitted_at[b]) * (1.0 / 3.0) - 0.5 * first
    acc = jnp.zeros((TILE, LANES), jnp.float32)

    def fit(acc, b, c, final):
        rows = slice(c * TILE, (c + 1) * TILE)
        change = final - change_at[b, rows]
        fitted_at[b, rows] = fitted_at[b, rows] + (1.0 / 3.0 + 0.5) * final
        change_at[b, rows] = change
        return acc + change * change

    for n, c in ((0, 2), (None, 0), (1, 1)):
        if n is None:
            for copy in sent[-1]:
                copy.wait_recv()
        else:
            for copy in pairs[n][phases - 1]:
                copy.wait_recv()
        for b in range(blocks):
            if n is None:
                final = direct(MICRO_SPELLS - 1, b, 0, TILE)
            else:
                final = paired(n, b)
            acc = fit(acc, b, c, final)
    squares[me_s] = acc
    copies = []
    for k in range(1, slabs):
        copies.append(
            pltpu.make_async_remote_copy(
                src_ref=squares.at[me_s],
                dst_ref=squares.at[me_s],
                send_sem=sq_send.at[k - 1],
                recv_sem=sq_recv.at[k - 1],
                device_id={"slab": lax.rem(me_s + k, slabs)},
                device_id_type=MESH,
            )
        )
    for copy in copies:
        copy.start()
    for copy in copies:
        copy.wait_recv()
    total = jnp.sum(jnp.sum(squares[...], axis=0), axis=(0, 1), keepdims=True)
    mean_square = total * (1.0 / (height * width * slabs))
    gain = step_cap / jnp.sqrt(mean_square + 1e-06)

    for c in range(chunks):
        here = slice(c * TILE, (c + 1) * TILE)
        rows = pl.ds(natural(c), TILE)
        for b in range(blocks):
            cols = slice(b * LANES, (b + 1) * LANES)
            if c == 0:
                density = gathered[MICRO_SPELLS - 1, me_e, b, pl.ds(front, TILE), :]
            else:
                density = partial[2 - c, 0, b]
            projected = fitted_at[b, here, :] + gain * change_at[b, here, :]
            projected_out[rows, cols] = flip(projected)
            scale_out[rows, cols] = flip(projected / density)

    for group_of in [[near], far, copies] + sent + pairs[0] + pairs[1] + pairs[2]:
        for copy in group_of:
            copy.wait_send()


def lift(finals, scale, projected, lifted_out, projected_out, scaled, sem):
    copies = [pltpu.make_async_copy(projected, projected_out, sem.at[9])]
    copies[0].start()
    for i in range(9):
        scaled[i] = finals[i] * scale[...]
        copy = pltpu.make_async_copy(scaled.at[i], lifted_out.at[0, i], sem.at[i])
        copy.start()
        copies.append(copy)
    for copy in copies:
        copy.wait()


def on_device(density0, relax_rate, perturbation):
    height, width = density0.shape
    ens, slabs = lax.axis_size("ens"), lax.axis_size("slab")
    assert perturbation.shape[0] == 1 and width % LANES == 0
    assert height == TOTAL and height % TILE == 0 and slabs % 2 == 0
    blocks = width // LANES
    rows = 3 * height
    phases = ens.bit_length() - 1
    assert ens == 2**phases
    chunks = height // TILE
    assert chunks == 3
    f32 = jnp.float32
    field = jax.ShapeDtypeStruct((height, width), f32)
    vmem = pl.BlockSpec(memory_space=pltpu.VMEM)
    hbm = pl.BlockSpec(memory_space=pltpu.HBM)
    dma = pltpu.SemaphoreType.DMA
    finals, scale, projected = pl.pallas_call(
        functools.partial(kernel, ens, slabs),
        out_shape=(
            jax.ShapeDtypeStruct((9, height, width), f32),
            field,
            field,
        ),
        in_specs=[hbm] * 3,
        out_specs=[vmem] * 3,
        scratch_shapes=[
            pltpu.VMEM((height, width), f32),
            pltpu.VMEM((height, width), jnp.int32),
            pltpu.VMEM((3, 2, height, width), f32),
            pltpu.VMEM((9, blocks, rows, LANES), f32),
            pltpu.VMEM((9, blocks, rows, LANES), f32),
            pltpu.VMEM((3, blocks, rows, LANES), f32),
            pltpu.VMEM((MICRO_SPELLS, ens, blocks, rows, LANES), f32),
            pltpu.VMEM((3, phases, blocks, TILE, LANES), f32),
            pltpu.VMEM((3, phases, blocks, TILE, LANES), f32),
            pltpu.VMEM((blocks, height, LANES), f32),
            pltpu.VMEM((blocks, height, LANES), f32),
            pltpu.VMEM((slabs, TILE, LANES), f32),
            dma((3,)),
            dma(()),
            dma(()),
            dma((chunks,)),
            dma((chunks,)),
            dma((PIECES, ens - 1)),
            dma((PIECES, ens - 1)),
            dma((3, phases, phases)),
            dma((3, phases, phases)),
            dma((slabs - 1,)),
            dma((slabs - 1,)),
        ],
        compiler_params=pltpu.CompilerParams(
            collective_id=0, has_side_effects=True, vmem_limit_bytes=48 << 20
        ),
    )(*(pltpu.with_memory_space_constraint(x, pltpu.HBM) for x in (density0, relax_rate, perturbation)))
    return pl.pallas_call(
        lift,
        out_shape=(jax.ShapeDtypeStruct((1, 9, height, width), f32), field),
        in_specs=[vmem] * 3,
        out_specs=[hbm] * 2,
        scratch_shapes=[pltpu.VMEM((9, height, width), f32), dma((10,))],
        compiler_params=pltpu.CompilerParams(vmem_limit_bytes=2 << 20),
    )(finals, scale, projected)


def solution(mesh):
    in_specs = (P("slab", None), P("slab", None), P("ens", "slab", None))
    out_specs = (P("ens", None, "slab", None), P("slab", None))
    return jax.shard_map(
        on_device, mesh=mesh, in_specs=in_specs, out_specs=out_specs, check_vma=False
    )
```

```python
import functools

import jax
import jax.numpy as jnp
from jax import lax
from jax.experimental import pallas as pl
from jax.experimental.pallas import tpu as pltpu
from jax.sharding import PartitionSpec as P

MICRO_SPELLS = 3
STEPS = 8
TOTAL = MICRO_SPELLS * STEPS
LANES = 128
TILE = 8
WIDE = 4

row_moves = (0, 0, 1, 0, -1, 1, 1, -1, -1)
col_moves = (0, 1, 0, -1, 0, 1, -1, -1, 1)
mirrored = (0, 1, 4, 3, 2, 8, 7, 6, 5)
lattice_weights = (4.0 / 9.0,) + (1.0 / 9.0,) * 4 + (1.0 / 36.0,) * 4
shift_amp = 0.08
step_cap = 0.25
MESH = pl.DeviceIdType.MESH
OWN, NEAR, FAR = 0, 1, 2
DUMMY = MICRO_SPELLS - 1


def collide(f, keep, third, ninth):
    plus = f[1] + (f[5] + f[8])
    minus = f[3] + (f[6] + f[7])
    density = (f[0] + (f[2] + f[4])) + (plus + minus)
    mom_col = plus - minus
    mom_row = (f[2] - f[4]) + ((f[5] + f[6]) - (f[7] + f[8]))
    inverse = 1.5 / density
    vel_row = mom_row * inverse
    vel_col = mom_col * inverse
    third_row = third * mom_row
    third_col = third * mom_col
    half_rr = third_row * vel_row
    half_cc = third_col * vel_col
    quarter_rc = (third_row * vel_col) * 0.5
    squares = half_rr + half_cc
    base = ninth * density - squares * (1.0 / 3.0)
    even_col = base + half_cc
    even_row = base + half_rr
    corner = 0.25 * (base + squares)
    even_57 = corner + quarter_rc
    even_68 = corner - quarter_rc
    odd_57 = 0.25 * (third_row + third_col)
    odd_68 = 0.25 * (third_row - third_col)
    out = (
        keep * f[0] + 4.0 * base,
        keep * f[1] + (even_col + third_col),
        keep * f[2] + (even_row + third_row),
        keep * f[3] + (even_col - third_col),
        keep * f[4] + (even_row - third_row),
        keep * f[5] + (even_57 + odd_57),
        keep * f[6] + (even_68 + odd_68),
        keep * f[7] + (even_57 - odd_57),
        keep * f[8] + (even_68 - odd_68),
    )
    return out, density


def kernel(
    ens,
    slabs,
    density_hbm,
    relax_hbm,
    pert_hbm,
    finals,
    scale_out,
    projected_out,
    density_in,
    pert_in,
    raws,
    even,
    odd,
    coef,
    gathered,
    partial,
    received,
    change_at,
    fitted_at,
    squares,
    in_sem,
    halo_send,
    near_recv,
    far_recv,
    ens_send,
    ens_recv,
    pair_send,
    ahead_recv,
    tail_recv,
    sq_send,
    sq_recv,
):
    height, width = density_in.shape
    blocks = width // LANES
    chunks = height // TILE
    wide = WIDE if blocks % WIDE == 0 else 1
    phases = ens.bit_length() - 1
    me_e = lax.axis_index("ens")
    me_s = lax.axis_index("slab")
    flipped = lax.rem(me_s, 2)

    barrier = pltpu.get_barrier_semaphore()
    for k in range(1, ens):
        pl.semaphore_signal(
            barrier, inc=1, device_id={"ens": lax.rem(me_e + k, ens)}, device_id_type=MESH
        )
    for k in range(1, slabs):
        pl.semaphore_signal(
            barrier, inc=1, device_id={"slab": lax.rem(me_s + k, slabs)}, device_id_type=MESH
        )

    loads = [
        pltpu.make_async_copy(density_hbm, density_in, in_sem.at[0]),
        pltpu.make_async_copy(pert_hbm.at[0], pert_in, in_sem.at[1]),
        pltpu.make_async_copy(relax_hbm, raws.at[OWN, 1], in_sem.at[2]),
    ]
    for copy in loads:
        copy.start()

    lane = lax.broadcasted_iota(jnp.int32, (TILE, LANES), 1)
    sublane = lax.broadcasted_iota(jnp.int32, (TILE, LANES), 0)
    order = jnp.where(flipped == 1, TILE - 1 - sublane, sublane)
    edges = {1: lane == 0, -1: lane == LANES - 1}
    bodies = {1: lane != 0, -1: lane != LANES - 1}

    def drain(ref, sem):
        pltpu.make_async_copy(ref, ref, sem).wait()

    def flip(x):
        return jnp.take_along_axis(x, order, axis=0, mode="promise_in_bounds")

    def natural(c):
        return pl.multiple_of(TILE * jnp.where(flipped == 1, chunks - 1 - c, c), TILE)

    def moved_store(ref, at, first, x, move):
        count = x.shape[0]
        over = lambda mask, n: jnp.broadcast_to(mask[None], (n, TILE, LANES))
        turned = pltpu.roll(x, 1 if move == 1 else LANES - 1, 2)
        pltpu.store(
            ref.at[pl.ds(first, count), at, :], turned, mask=over(bodies[move], count)
        )
        edge = edges[move]
        low = first + move
        if low < 0:
            pltpu.store(ref.at[pl.ds(blocks - 1, 1), at, :], turned[:1], mask=over(edge, 1))
            turned, low, count = turned[1:], 0, count - 1
        elif low + count > blocks:
            pltpu.store(ref.at[pl.ds(0, 1), at, :], turned[count - 1 :], mask=over(edge, 1))
            turned, count = turned[: count - 1], count - 1
        if count:
            pltpu.store(ref.at[pl.ds(low, count), at, :], turned, mask=over(edge, count))

    def fill(place, offset, which):
        for c in which:
            at = pl.ds(offset + c * TILE, TILE)
            rows = pl.ds(natural(c), TILE)
            for b in range(blocks):
                cols = slice(b * LANES, (b + 1) * LANES)
                rate = flip(raws[place, 1, rows, cols])
                fresh = flip(raws[place, 0, rows, cols])
                coef[0, b, at, :] = 1.0 - rate
                coef[1, b, at, :] = rate * (1.0 / 3.0)
                coef[2, b, at, :] = rate * (1.0 / 9.0)
                for weight, members in (
                    (lattice_weights[0], (0,)),
                    (lattice_weights[1], (1, 2, 3, 4)),
                    (lattice_weights[5], (5, 6, 7, 8)),
                ):
                    part = weight * fresh
                    for i in members:
                        if col_moves[i] == 0:
                            odd[i, b, at, :] = part
                        else:
                            moved_store(odd.at[i], at, b, part[None], col_moves[i])

    front = height

    def group(k, low, slot=None):
        source, dest = (odd, even) if k % 2 == 0 else (even, odd)
        at = front + low
        rows = pl.ds(at, TILE)
        for first in range(0, blocks, wide):
            cols = pl.ds(first, wide)
            f = [source[i, cols, pl.ds(at - row_moves[i], TILE), :] for i in range(9)]
            out, density = collide(f, *(coef[n, cols, rows, :] for n in range(3)))
            if slot is not None:
                gathered[slot, me_e, cols, rows, :] = density
            for i in range(9):
                if col_moves[i] == 0:
                    dest[i, cols, rows, :] = out[i]
                else:
                    moved_store(dest.at[i], rows, first, out[i], col_moves[i])

    for copy in loads:
        copy.wait()
    for c in range(chunks):
        rows = slice(c * TILE, (c + 1) * TILE)
        raws[OWN, 0, rows, :] = density_in[rows, :] + shift_amp * pert_in[rows, :].astype(
            jnp.float32
        )
    fill(OWN, front, range(chunks))

    def triangle(k):
        low, high = k - 1, height + 1 - k
        for first in range(low, high, TILE):
            group(k, min(first, high - TILE), 0 if k == STEPS + 1 else None)

    triangle(2)
    triangle(3)
    pl.semaphore_wait(barrier, ens + slabs - 2)
    near_to = me_s + 1 - 2 * flipped
    far_to = lax.rem(me_s + slabs - 1 + 2 * flipped, slabs)
    far = []
    for c in range(chunks):
        rows = pl.ds(natural(c), TILE)
        far.append(
            pltpu.make_async_remote_copy(
                src_ref=raws.at[OWN, :, rows],
                dst_ref=raws.at[FAR, :, rows],
                send_sem=halo_send,
                recv_sem=far_recv.at[c],
                device_id={"slab": far_to},
                device_id_type=MESH,
            )
        )
    near = pltpu.make_async_remote_copy(
        src_ref=raws.at[OWN],
        dst_ref=raws.at[NEAR],
        send_sem=halo_send,
        recv_sem=near_recv,
        device_id={"slab": near_to},
        device_id_type=MESH,
    )
    near.start()
    for copy in far:
        copy.start()
    for k in range(4, STEPS + 2):
        triangle(k)

    near.wait_recv()
    fill(NEAR, front + height, range(chunks))

    def lean(t, base):
        for n in range(4):
            for j in range(chunks):
                slot = jnp.where(t == 1, 0, DUMMY) if n == 3 else None
                group(n % 2, base + (TILE * j - n), slot)
        return base - 4

    def differing(mask):
        peer = me_e
        for n in range(phases):
            if mask >> n & 1:
                peer = peer + 2**n - 2 ** (n + 1) * lax.rem(me_e // 2**n, 2)
        return peer

    def send(spell, low, high):
        own = pl.ds(front + low, high - low)
        for k in sorted(range(1, ens), key=lambda k: -k.bit_count()):
            pltpu.make_async_remote_copy(
                src_ref=gathered.at[spell, me_e, :, own],
                dst_ref=gathered.at[spell, me_e, :, own],
                send_sem=ens_send,
                recv_sem=ens_recv.at[spell // (MICRO_SPELLS - 1)],
                device_id={"ens": differing(k)},
                device_id_type=MESH,
            ).start()

    def sent_bytes(rows):
        return gathered.at[0, pl.ds(0, ens - 1), :, pl.ds(0, rows)]

    def near_side(k):
        count = 2 * height + 2 - 2 * k
        for j in range((count + TILE - 1) // TILE - 1, -1, -1):
            group(k, k - 1 + TILE * j, sample.get(k))

    def strip(m, k):
        if 2 <= k <= TOTAL:
            group(k, k - 1 - TILE * m, sample.get(k))

    def arrived(c):
        far[c].wait_recv()
        fill(FAR, front - height, (chunks - 1 - c,))

    def settle(b, c):
        at = front + c * TILE
        total = last[0, b, pl.ds(at, TILE), :]
        for i in range(1, 9):
            total = total + last[i, b, pl.ds(at - row_moves[i], TILE), :]
        return total

    cuts = [blocks * p // phases for p in range(phases + 1)]

    def pair(n, q, p):
        peer = differing(2 ** ((p + q) % phases))
        part = pl.ds(cuts[p], cuts[p + 1] - cuts[p])
        if n == 1:
            arrival = tail_recv.at[min(q * phases + p, (phases - 1) * phases)]
        else:
            arrival = ahead_recv.at[q]
        return pltpu.make_async_remote_copy(
            src_ref=partial.at[n, q, part],
            dst_ref=received.at[n, q, part],
            send_sem=pair_send,
            recv_sem=arrival,
            device_id={"ens": peer},
            device_id_type=MESH,
        )

    pairs = [[[pair(n, q, p) for p in range(phases)] for q in range(phases)] for n in range(3)]

    def send_pairs(n, c):
        for b in range(blocks):
            partial[n, 0, b] = settle(b, c)
        for copy in pairs[n][0]:
            copy.start()

    last = even if TOTAL % 2 == 0 else odd
    sample = {STEPS + 1: 0, 2 * STEPS + 1: 1}
    lax.fori_loop(0, 2, lean, height - 1)
    send(0, STEPS, height)
    for k in range(STEPS + 2, STEPS + 5):
        near_side(k)
    arrived(0)
    for n in range(TOTAL + 11):
        if n == 7:
            send(1, 2 * STEPS, height)
            arrived(1)
        if n == 12:
            send(0, 0, STEPS)
            arrived(2)
        if n == 16:
            send(1, STEPS, 2 * STEPS)
        if n == 23:
            for b in range(blocks):
                partial[2, 0, b] = gathered[1, me_e, b, pl.ds(front, TILE), :]
            send_pairs(0, 2)
            for copy in pairs[2][0]:
                copy.start()
        if n == 30:
            send_pairs(1, 1)
        if STEPS + 5 + n <= TOTAL:
            near_side(STEPS + 5 + n)
        strip(1, n + 2)
        strip(2, n - 5)
        strip(3, n - 10)
    for b in range(blocks):
        gathered[MICRO_SPELLS - 1, me_e, b, pl.ds(front, TILE), :] = settle(b, 0)
    send(MICRO_SPELLS - 1, 0, TILE)

    def put_finals(c, carry):
        at = front + c * TILE
        rows = pl.ds(natural(c), TILE)
        for i in range(9):
            to = jnp.where(flipped == 1, mirrored[i], i)
            for b in range(blocks):
                cols = slice(b * LANES, (b + 1) * LANES)
                finals[to, rows, cols] = flip(last[i, b, pl.ds(at - row_moves[i], TILE), :])
        return carry

    lax.fori_loop(0, chunks, put_finals, 0)

    def direct(spell, b, low, count):
        at = pl.ds(front + low, count)
        total = gathered[spell, 0, b, at, :]
        for member in range(1, ens):
            total = total + gathered[spell, member, b, at, :]
        return total * (1.0 / ens)

    def paired(n, b):
        return (partial[n, phases - 1, b] + received[n, phases - 1, b]) * (1.0 / ens)

    def pass_on(q, n, p):
        part = slice(cuts[p], cuts[p + 1])
        partial[n, q + 1, part] = partial[n, q, part] + received[n, q, part]
        pairs[n][q + 1][p].start()

    ahead_bytes = partial.at[pl.ds(0, 2), 0]

    def early(b, carry):
        change_at[b] = direct(0, b, 0, height)
        fitted_at[b, pl.ds(TILE, height - TILE), :] = direct(1, b, TILE, height - TILE)
        return carry

    for q in range(phases - 1):
        drain(ahead_bytes, ahead_recv.at[q])
        for n in (0, 2):
            for p in range(phases):
                pass_on(q, n, p)
    drain(sent_bytes(2 * height - TILE), ens_recv.at[0])
    lax.fori_loop(0, blocks, early, 0)
    for q in range(phases - 1):
        for p in range(phases):
            pairs[1][q][p].wait_recv()
            pass_on(q, 1, p)
    drain(ahead_bytes, ahead_recv.at[phases - 1])
    for b in range(blocks):
        fitted_at[b, 0:TILE] = paired(2, b)
    for b in range(blocks):
        first = change_at[b]
        fitted_at[b] = (first + fitted_at[b]) * (1.0 / 3.0) - 0.5 * first
    acc = jnp.zeros((TILE, LANES), jnp.float32)

    def fit(acc, b, c, final):
        rows = slice(c * TILE, (c + 1) * TILE)
        change = final - change_at[b, rows]
        fitted_at[b, rows] = fitted_at[b, rows] + (1.0 / 3.0 + 0.5) * final
        change_at[b, rows] = change
        return acc + change * change

    for n, c in ((0, 2), (None, 0), (1, 1)):
        if n is None:
            drain(sent_bytes(TILE), ens_recv.at[1])
        if n == 1:
            drain(partial.at[1, 0], tail_recv.at[(phases - 1) * phases])
        for b in range(blocks):
            if n is None:
                final = direct(MICRO_SPELLS - 1, b, 0, TILE)
            else:
                final = paired(n, b)
            acc = fit(acc, b, c, final)
    squares[me_s] = jnp.sum(acc, axis=0, keepdims=True)
    copies = []
    for k in range(1, slabs):
        copies.append(
            pltpu.make_async_remote_copy(
                src_ref=squares.at[me_s],
                dst_ref=squares.at[me_s],
                send_sem=sq_send,
                recv_sem=sq_recv,
                device_id={"slab": lax.rem(me_s + k, slabs)},
                device_id_type=MESH,
            )
        )
    for copy in copies:
        copy.start()
    for c in range(chunks):
        here = slice(c * TILE, (c + 1) * TILE)
        rows = pl.ds(natural(c), TILE)
        for b in range(blocks):
            cols = slice(b * LANES, (b + 1) * LANES)
            if c == 0:
                density = gathered[MICRO_SPELLS - 1, me_e, b, pl.ds(front, TILE), :]
            else:
                density = partial[2 - c, 0, b]
            projected_out[rows, cols] = flip(fitted_at[b, here, :])
            density_in[rows, cols] = flip(change_at[b, here, :])
            scale_out[rows, cols] = flip(1.0 / density)
    drain(squares.at[pl.ds(0, slabs - 1)], sq_recv)
    total = jnp.sum(jnp.sum(squares[...], axis=0), axis=(0, 1), keepdims=True)
    mean_square = total * (1.0 / (height * width * slabs))
    gain = step_cap / jnp.sqrt(mean_square + 1e-06)
    for c in range(chunks):
        rows = slice(c * TILE, (c + 1) * TILE)
        projected = projected_out[rows, :] + gain * density_in[rows, :]
        projected_out[rows, :] = projected
        scale_out[rows, :] = projected * scale_out[rows, :]

    drain(raws.at[pl.ds(0, 2)], halo_send)
    drain(sent_bytes(2 * height), ens_send)
    drain(partial, pair_send)
    drain(squares.at[pl.ds(0, slabs - 1)], sq_send)


def lift(finals, scale, projected, lifted_out, projected_out, scaled, sem):
    small = pltpu.make_async_copy(projected, projected_out, sem.at[1])
    small.start()
    for i in range(9):
        scaled[i] = finals[i] * scale[...]
        pltpu.make_async_copy(scaled.at[i], lifted_out.at[0, i], sem.at[0]).start()
    pltpu.make_async_copy(scaled, lifted_out.at[0], sem.at[0]).wait()
    small.wait()


def on_device(density0, relax_rate, perturbation):
    height, width = density0.shape
    ens, slabs = lax.axis_size("ens"), lax.axis_size("slab")
    assert perturbation.shape[0] == 1 and width % LANES == 0
    assert height == TOTAL and height % TILE == 0 and slabs % 2 == 0
    blocks = width // LANES
    rows = 3 * height
    phases = ens.bit_length() - 1
    assert ens == 2**phases
    chunks = height // TILE
    assert chunks == 3
    f32 = jnp.float32
    field = jax.ShapeDtypeStruct((height, width), f32)
    vmem = pl.BlockSpec(memory_space=pltpu.VMEM)
    hbm = pl.BlockSpec(memory_space=pltpu.HBM)
    dma = pltpu.SemaphoreType.DMA
    finals, scale, projected = pl.pallas_call(
        functools.partial(kernel, ens, slabs),
        out_shape=(
            jax.ShapeDtypeStruct((9, height, width), f32),
            field,
            field,
        ),
        in_specs=[hbm] * 3,
        out_specs=[vmem] * 3,
        scratch_shapes=[
            pltpu.VMEM((height, width), f32),
            pltpu.VMEM((height, width), jnp.int32),
            pltpu.VMEM((3, 2, height, width), f32),
            pltpu.VMEM((9, blocks, rows, LANES), f32),
            pltpu.VMEM((9, blocks, rows, LANES), f32),
            pltpu.VMEM((3, blocks, rows, LANES), f32),
            pltpu.VMEM((MICRO_SPELLS, ens, blocks, rows, LANES), f32),
            pltpu.VMEM((3, phases, blocks, TILE, LANES), f32),
            pltpu.VMEM((3, phases, blocks, TILE, LANES), f32),
            pltpu.VMEM((blocks, height, LANES), f32),
            pltpu.VMEM((blocks, height, LANES), f32),
            pltpu.VMEM((slabs, 1, LANES), f32),
            dma((3,)),
            dma(()),
            dma(()),
            dma((chunks,)),
            dma(()),
            dma((2,)),
            dma(()),
            dma((phases,)),
            dma(((phases - 1) * phases + 1,)),
            dma(()),
            dma(()),
        ],
        compiler_params=pltpu.CompilerParams(
            collective_id=0, has_side_effects=True, vmem_limit_bytes=48 << 20
        ),
    )(*(pltpu.with_memory_space_constraint(x, pltpu.HBM) for x in (density0, relax_rate, perturbation)))
    return pl.pallas_call(
        lift,
        out_shape=(jax.ShapeDtypeStruct((1, 9, height, width), f32), field),
        in_specs=[vmem] * 3,
        out_specs=[hbm] * 2,
        scratch_shapes=[pltpu.VMEM((9, height, width), f32), dma((2,))],
        compiler_params=pltpu.CompilerParams(vmem_limit_bytes=2 << 20),
    )(finals, scale, projected)


def solution(mesh):
    in_specs = (P("slab", None), P("slab", None), P("ens", "slab", None))
    out_specs = (P("ens", None, "slab", None), P("slab", None))
    return jax.shard_map(
        on_device, mesh=mesh, in_specs=in_specs, out_specs=out_specs, check_vma=False
    )
```

```python
import functools

import jax
import jax.numpy as jnp
from jax import lax
from jax.experimental import pallas as pl
from jax.experimental.pallas import tpu as pltpu
from jax.sharding import PartitionSpec as P

MICRO_SPELLS = 3
STEPS = 8
TOTAL = MICRO_SPELLS * STEPS
LANES = 128
TILE = 8
WIDE = 4

row_moves = (0, 0, 1, 0, -1, 1, 1, -1, -1)
col_moves = (0, 1, 0, -1, 0, 1, -1, -1, 1)
mirrored = (0, 1, 4, 3, 2, 8, 7, 6, 5)
lattice_weights = (4.0 / 9.0,) + (1.0 / 9.0,) * 4 + (1.0 / 36.0,) * 4
shift_amp = 0.08
step_cap = 0.25
MESH = pl.DeviceIdType.MESH
OWN, NEAR, FAR = 0, 1, 2
DUMMY = MICRO_SPELLS - 1


def collide(f, keep, third, ninth):
    plus = f[1] + (f[5] + f[8])
    minus = f[3] + (f[6] + f[7])
    density = (f[0] + (f[2] + f[4])) + (plus + minus)
    mom_col = plus - minus
    mom_row = (f[2] - f[4]) + ((f[5] + f[6]) - (f[7] + f[8]))
    inverse = 1.5 / density
    vel_row = mom_row * inverse
    vel_col = mom_col * inverse
    third_row = third * mom_row
    third_col = third * mom_col
    half_rr = third_row * vel_row
    half_cc = third_col * vel_col
    quarter_rc = (third_row * vel_col) * 0.5
    squares = half_rr + half_cc
    base = ninth * density - squares * (1.0 / 3.0)
    even_col = base + half_cc
    even_row = base + half_rr
    corner = 0.25 * (base + squares)
    even_57 = corner + quarter_rc
    even_68 = corner - quarter_rc
    odd_57 = 0.25 * (third_row + third_col)
    odd_68 = 0.25 * (third_row - third_col)
    out = (
        keep * f[0] + 4.0 * base,
        keep * f[1] + (even_col + third_col),
        keep * f[2] + (even_row + third_row),
        keep * f[3] + (even_col - third_col),
        keep * f[4] + (even_row - third_row),
        keep * f[5] + (even_57 + odd_57),
        keep * f[6] + (even_68 + odd_68),
        keep * f[7] + (even_57 - odd_57),
        keep * f[8] + (even_68 - odd_68),
    )
    return out, density


def kernel(
    ens,
    slabs,
    density_hbm,
    relax_hbm,
    pert_hbm,
    finals,
    scale_out,
    projected_out,
    density_in,
    pert_in,
    raws,
    even,
    odd,
    coef,
    gathered,
    partial,
    received,
    change_at,
    fitted_at,
    squares,
    in_sem,
    halo_send,
    near_recv,
    far_recv,
    ens_send,
    ens_recv,
    pair_send,
    ahead_recv,
    tail_recv,
    sq_send,
    sq_recv,
):
    height, width = density_in.shape
    blocks = width // LANES
    chunks = height // TILE
    wide = WIDE if blocks % WIDE == 0 else 1
    phases = ens.bit_length() - 1
    me_e = lax.axis_index("ens")
    me_s = lax.axis_index("slab")
    flipped = lax.rem(me_s, 2)

    barrier = pltpu.get_barrier_semaphore()
    for k in range(1, ens):
        pl.semaphore_signal(
            barrier, inc=1, device_id={"ens": lax.rem(me_e + k, ens)}, device_id_type=MESH
        )
    for k in range(1, slabs):
        pl.semaphore_signal(
            barrier, inc=1, device_id={"slab": lax.rem(me_s + k, slabs)}, device_id_type=MESH
        )

    loads = [
        pltpu.make_async_copy(density_hbm, density_in, in_sem.at[0]),
        pltpu.make_async_copy(pert_hbm.at[0], pert_in, in_sem.at[1]),
        pltpu.make_async_copy(relax_hbm, raws.at[OWN, 1], in_sem.at[2]),
    ]
    for copy in loads:
        copy.start()

    lane = lax.broadcasted_iota(jnp.int32, (TILE, LANES), 1)
    sublane = lax.broadcasted_iota(jnp.int32, (TILE, LANES), 0)
    order = jnp.where(flipped == 1, TILE - 1 - sublane, sublane)
    edges = {1: lane == 0, -1: lane == LANES - 1}
    bodies = {1: lane != 0, -1: lane != LANES - 1}

    def drain(ref, sem):
        pltpu.make_async_copy(ref, ref, sem).wait()

    def flip(x):
        return jnp.take_along_axis(x, order, axis=0, mode="promise_in_bounds")

    def natural(c):
        return pl.multiple_of(TILE * jnp.where(flipped == 1, chunks - 1 - c, c), TILE)

    def moved_store(ref, at, first, x, move):
        count = x.shape[0]
        over = lambda mask, n: jnp.broadcast_to(mask[None], (n, TILE, LANES))
        turned = pltpu.roll(x, 1 if move == 1 else LANES - 1, 2)
        pltpu.store(
            ref.at[pl.ds(first, count), at, :], turned, mask=over(bodies[move], count)
        )
        edge = edges[move]
        low = first + move
        if low < 0:
            pltpu.store(ref.at[pl.ds(blocks - 1, 1), at, :], turned[:1], mask=over(edge, 1))
            turned, low, count = turned[1:], 0, count - 1
        elif low + count > blocks:
            pltpu.store(ref.at[pl.ds(0, 1), at, :], turned[count - 1 :], mask=over(edge, 1))
            turned, count = turned[: count - 1], count - 1
        if count:
            pltpu.store(ref.at[pl.ds(low, count), at, :], turned, mask=over(edge, count))

    def fill(place, offset, which):
        for c in which:
            at = pl.ds(offset + c * TILE, TILE)
            rows = pl.ds(natural(c), TILE)
            for b in range(blocks):
                cols = slice(b * LANES, (b + 1) * LANES)
                rate = flip(raws[place, 1, rows, cols])
                fresh = flip(raws[place, 0, rows, cols])
                coef[0, b, at, :] = 1.0 - rate
                coef[1, b, at, :] = rate * (1.0 / 3.0)
                coef[2, b, at, :] = rate * (1.0 / 9.0)
                for weight, members in (
                    (lattice_weights[0], (0,)),
                    (lattice_weights[1], (1, 2, 3, 4)),
                    (lattice_weights[5], (5, 6, 7, 8)),
                ):
                    part = weight * fresh
                    for i in members:
                        if col_moves[i] == 0:
                            odd[i, b, at, :] = part
                        else:
                            moved_store(odd.at[i], at, b, part[None], col_moves[i])

    front = height

    def group(k, low, slot=None):
        source, dest = (odd, even) if k % 2 == 0 else (even, odd)
        at = front + low
        rows = pl.ds(at, TILE)
        for first in range(0, blocks, wide):
            cols = pl.ds(first, wide)
            f = [source[i, cols, pl.ds(at - row_moves[i], TILE), :] for i in range(9)]
            out, density = collide(f, *(coef[n, cols, rows, :] for n in range(3)))
            if slot is not None:
                gathered[slot, me_e, cols, rows, :] = density
            for i in range(9):
                if col_moves[i] == 0:
                    dest[i, cols, rows, :] = out[i]
                else:
                    moved_store(dest.at[i], rows, first, out[i], col_moves[i])

    for copy in loads:
        copy.wait()
    for c in range(chunks):
        rows = slice(c * TILE, (c + 1) * TILE)
        raws[OWN, 0, rows, :] = density_in[rows, :] + shift_amp * pert_in[rows, :].astype(
            jnp.float32
        )
    fill(OWN, front, range(chunks))

    def triangle(k):
        low, high = k - 1, height + 1 - k
        for first in range(low, high, TILE):
            group(k, min(first, high - TILE), 0 if k == STEPS + 1 else None)

    triangle(2)
    triangle(3)
    pl.semaphore_wait(barrier, ens + slabs - 2)
    near_to = me_s + 1 - 2 * flipped
    far_to = lax.rem(me_s + slabs - 1 + 2 * flipped, slabs)
    far = []
    for c in range(chunks):
        rows = pl.ds(natural(c), TILE)
        far.append(
            pltpu.make_async_remote_copy(
                src_ref=raws.at[OWN, :, rows],
                dst_ref=raws.at[FAR, :, rows],
                send_sem=halo_send,
                recv_sem=far_recv.at[c],
                device_id={"slab": far_to},
                device_id_type=MESH,
            )
        )
    near = pltpu.make_async_remote_copy(
        src_ref=raws.at[OWN],
        dst_ref=raws.at[NEAR],
        send_sem=halo_send,
        recv_sem=near_recv,
        device_id={"slab": near_to},
        device_id_type=MESH,
    )
    near.start()
    for copy in far:
        copy.start()
    for k in range(4, STEPS + 2):
        triangle(k)

    def differing(mask):
        peer = me_e
        for n in range(phases):
            if mask >> n & 1:
                peer = peer + 2**n - 2 ** (n + 1) * lax.rem(me_e // 2**n, 2)
        return peer

    def send(spell, low, high):
        own = pl.ds(front + low, high - low)
        for k in sorted(range(1, ens), key=lambda k: -k.bit_count()):
            pltpu.make_async_remote_copy(
                src_ref=gathered.at[spell, me_e, :, own],
                dst_ref=gathered.at[spell, me_e, :, own],
                send_sem=ens_send,
                recv_sem=ens_recv.at[spell // (MICRO_SPELLS - 1)],
                device_id={"ens": differing(k)},
                device_id_type=MESH,
            ).start()

    send(0, STEPS, 2 * STEPS)
    near.wait_recv()
    fill(NEAR, front + height, range(chunks))

    def lean(t, base):
        for n in range(4):
            for j in range(chunks):
                slot = jnp.where(t == 1, 0, DUMMY) if n == 3 else None
                group(n % 2, base + (TILE * j - n), slot)
        return base - 4

    def sent_bytes(rows):
        return gathered.at[0, pl.ds(0, ens - 1), :, pl.ds(0, rows)]

    def near_side(k):
        count = 2 * height + 2 - 2 * k
        for j in range((count + TILE - 1) // TILE - 1, -1, -1):
            group(k, k - 1 + TILE * j, sample.get(k))

    def strip(m, k):
        if 2 <= k <= TOTAL:
            group(k, k - 1 - TILE * m, sample.get(k))

    def arrived(c):
        far[c].wait_recv()
        fill(FAR, front - height, (chunks - 1 - c,))

    def settle(b, c):
        at = front + c * TILE
        total = last[0, b, pl.ds(at, TILE), :]
        for i in range(1, 9):
            total = total + last[i, b, pl.ds(at - row_moves[i], TILE), :]
        return total

    cuts = [blocks * p // phases for p in range(phases + 1)]

    def pair(n, q, p):
        peer = differing(2 ** ((p + q) % phases))
        part = pl.ds(cuts[p], cuts[p + 1] - cuts[p])
        if n == 1:
            arrival = tail_recv.at[min(q * phases + p, (phases - 1) * phases)]
        else:
            arrival = ahead_recv.at[q]
        return pltpu.make_async_remote_copy(
            src_ref=partial.at[n, q, part],
            dst_ref=received.at[n, q, part],
            send_sem=pair_send,
            recv_sem=arrival,
            device_id={"ens": peer},
            device_id_type=MESH,
        )

    pairs = [[[pair(n, q, p) for p in range(phases)] for q in range(phases)] for n in range(3)]

    def send_pairs(n, c):
        for b in range(blocks):
            partial[n, 0, b] = settle(b, c)
        for copy in pairs[n][0]:
            copy.start()

    last = even if TOTAL % 2 == 0 else odd
    sample = {STEPS + 1: 0, 2 * STEPS + 1: 1}
    lax.fori_loop(0, 2, lean, height - 1)
    send(0, 2 * STEPS, height)
    ahead = 2 * STEPS + 2
    for k in range(STEPS + 2, ahead):
        near_side(k)
    send(1, 2 * STEPS, height)
    arrived(0)
    for n in range(TOTAL + 11):
        if n == 7:
            arrived(1)
        if n == 12:
            send(0, 0, STEPS)
            arrived(2)
        if n == 16:
            send(1, STEPS, 2 * STEPS)
        if n == 23:
            for b in range(blocks):
                partial[2, 0, b] = gathered[1, me_e, b, pl.ds(front, TILE), :]
            send_pairs(0, 2)
            for copy in pairs[2][0]:
                copy.start()
        if n == 30:
            send_pairs(1, 1)
        if ahead + n <= TOTAL:
            near_side(ahead + n)
        strip(1, n + 2)
        strip(2, n - 5)
        strip(3, n - 10)
    for b in range(blocks):
        gathered[MICRO_SPELLS - 1, me_e, b, pl.ds(front, TILE), :] = settle(b, 0)
    send(MICRO_SPELLS - 1, 0, TILE)

    def put_finals(c, carry):
        at = front + c * TILE
        rows = pl.ds(natural(c), TILE)
        for i in range(9):
            to = jnp.where(flipped == 1, mirrored[i], i)
            for b in range(blocks):
                cols = slice(b * LANES, (b + 1) * LANES)
                finals[to, rows, cols] = flip(last[i, b, pl.ds(at - row_moves[i], TILE), :])
        return carry

    lax.fori_loop(0, chunks, put_finals, 0)

    def direct(spell, b, low, count):
        at = pl.ds(front + low, count)
        total = gathered[spell, 0, b, at, :]
        for member in range(1, ens):
            total = total + gathered[spell, member, b, at, :]
        return total * (1.0 / ens)

    def paired(n, b):
        return (partial[n, phases - 1, b] + received[n, phases - 1, b]) * (1.0 / ens)

    def pass_on(q, n, p):
        part = slice(cuts[p], cuts[p + 1])
        partial[n, q + 1, part] = partial[n, q, part] + received[n, q, part]
        pairs[n][q + 1][p].start()

    ahead_bytes = partial.at[pl.ds(0, 2), 0]

    def early(b, carry):
        change_at[b] = direct(0, b, 0, height)
        fitted_at[b, pl.ds(TILE, height - TILE), :] = direct(1, b, TILE, height - TILE)
        return carry

    for q in range(phases - 1):
        drain(ahead_bytes, ahead_recv.at[q])
        for n in (0, 2):
            for p in range(phases):
                pass_on(q, n, p)
    drain(sent_bytes(2 * height - TILE), ens_recv.at[0])
    lax.fori_loop(0, blocks, early, 0)
    for q in range(phases - 1):
        for p in range(phases):
            pairs[1][q][p].wait_recv()
            pass_on(q, 1, p)
    drain(ahead_bytes, ahead_recv.at[phases - 1])
    for b in range(blocks):
        fitted_at[b, 0:TILE] = paired(2, b)
    for b in range(blocks):
        first = change_at[b]
        fitted_at[b] = (first + fitted_at[b]) * (1.0 / 3.0) - 0.5 * first
    acc = jnp.zeros((TILE, LANES), jnp.float32)

    def fit(acc, b, c, final):
        rows = slice(c * TILE, (c + 1) * TILE)
        change = final - change_at[b, rows]
        fitted_at[b, rows] = fitted_at[b, rows] + (1.0 / 3.0 + 0.5) * final
        change_at[b, rows] = change
        return acc + change * change

    for n, c in ((0, 2), (None, 0), (1, 1)):
        if n is None:
            drain(sent_bytes(TILE), ens_recv.at[1])
        if n == 1:
            drain(partial.at[1, 0], tail_recv.at[(phases - 1) * phases])
        for b in range(blocks):
            if n is None:
                final = direct(MICRO_SPELLS - 1, b, 0, TILE)
            else:
                final = paired(n, b)
            acc = fit(acc, b, c, final)
    squares[me_s] = jnp.sum(acc, axis=0, keepdims=True)
    copies = []
    for k in range(1, slabs):
        copies.append(
            pltpu.make_async_remote_copy(
                src_ref=squares.at[me_s],
                dst_ref=squares.at[me_s],
                send_sem=sq_send,
                recv_sem=sq_recv,
                device_id={"slab": lax.rem(me_s + k, slabs)},
                device_id_type=MESH,
            )
        )
    for copy in copies:
        copy.start()
    for c in range(chunks):
        here = slice(c * TILE, (c + 1) * TILE)
        rows = pl.ds(natural(c), TILE)
        for b in range(blocks):
            cols = slice(b * LANES, (b + 1) * LANES)
            if c == 0:
                density = gathered[MICRO_SPELLS - 1, me_e, b, pl.ds(front, TILE), :]
            else:
                density = partial[2 - c, 0, b]
            projected_out[rows, cols] = flip(fitted_at[b, here, :])
            density_in[rows, cols] = flip(change_at[b, here, :])
            scale_out[rows, cols] = flip(1.0 / density)
    drain(squares.at[pl.ds(0, slabs - 1)], sq_recv)
    total = jnp.sum(jnp.sum(squares[...], axis=0), axis=(0, 1), keepdims=True)
    mean_square = total * (1.0 / (height * width * slabs))
    gain = step_cap / jnp.sqrt(mean_square + 1e-06)
    for c in range(chunks):
        rows = slice(c * TILE, (c + 1) * TILE)
        projected = projected_out[rows, :] + gain * density_in[rows, :]
        projected_out[rows, :] = projected
        scale_out[rows, :] = projected * scale_out[rows, :]

    drain(raws.at[pl.ds(0, 2)], halo_send)
    drain(sent_bytes(2 * height), ens_send)
    drain(partial, pair_send)
    drain(squares.at[pl.ds(0, slabs - 1)], sq_send)


def lift(finals, scale, projected, lifted_out, projected_out, scaled, sem):
    small = pltpu.make_async_copy(projected, projected_out, sem.at[1])
    small.start()
    for i in range(9):
        scaled[i] = finals[i] * scale[...]
        pltpu.make_async_copy(scaled.at[i], lifted_out.at[0, i], sem.at[0]).start()
    pltpu.make_async_copy(scaled, lifted_out.at[0], sem.at[0]).wait()
    small.wait()


def on_device(density0, relax_rate, perturbation):
    height, width = density0.shape
    ens, slabs = lax.axis_size("ens"), lax.axis_size("slab")
    assert perturbation.shape[0] == 1 and width % LANES == 0
    assert height == TOTAL and height % TILE == 0 and slabs % 2 == 0
    blocks = width // LANES
    rows = 3 * height
    phases = ens.bit_length() - 1
    assert ens == 2**phases
    chunks = height // TILE
    assert chunks == 3
    f32 = jnp.float32
    field = jax.ShapeDtypeStruct((height, width), f32)
    vmem = pl.BlockSpec(memory_space=pltpu.VMEM)
    hbm = pl.BlockSpec(memory_space=pltpu.HBM)
    dma = pltpu.SemaphoreType.DMA
    finals, scale, projected = pl.pallas_call(
        functools.partial(kernel, ens, slabs),
        out_shape=(
            jax.ShapeDtypeStruct((9, height, width), f32),
            field,
            field,
        ),
        in_specs=[hbm] * 3,
        out_specs=[vmem] * 3,
        scratch_shapes=[
            pltpu.VMEM((height, width), f32),
            pltpu.VMEM((height, width), jnp.int32),
            pltpu.VMEM((3, 2, height, width), f32),
            pltpu.VMEM((9, blocks, rows, LANES), f32),
            pltpu.VMEM((9, blocks, rows, LANES), f32),
            pltpu.VMEM((3, blocks, rows, LANES), f32),
            pltpu.VMEM((MICRO_SPELLS, ens, blocks, rows, LANES), f32),
            pltpu.VMEM((3, phases, blocks, TILE, LANES), f32),
            pltpu.VMEM((3, phases, blocks, TILE, LANES), f32),
            pltpu.VMEM((blocks, height, LANES), f32),
            pltpu.VMEM((blocks, height, LANES), f32),
            pltpu.VMEM((slabs, 1, LANES), f32),
            dma((3,)),
            dma(()),
            dma(()),
            dma((chunks,)),
            dma(()),
            dma((2,)),
            dma(()),
            dma((phases,)),
            dma(((phases - 1) * phases + 1,)),
            dma(()),
            dma(()),
        ],
        compiler_params=pltpu.CompilerParams(
            collective_id=0, has_side_effects=True, vmem_limit_bytes=48 << 20
        ),
    )(*(pltpu.with_memory_space_constraint(x, pltpu.HBM) for x in (density0, relax_rate, perturbation)))
    return pl.pallas_call(
        lift,
        out_shape=(jax.ShapeDtypeStruct((1, 9, height, width), f32), field),
        in_specs=[vmem] * 3,
        out_specs=[hbm] * 2,
        scratch_shapes=[pltpu.VMEM((9, height, width), f32), dma((2,))],
        compiler_params=pltpu.CompilerParams(vmem_limit_bytes=2 << 20),
    )(finals, scale, projected)


def solution(mesh):
    in_specs = (P("slab", None), P("slab", None), P("ens", "slab", None))
    out_specs = (P("ens", None, "slab", None), P("slab", None))
    return jax.shard_map(
        on_device, mesh=mesh, in_specs=in_specs, out_specs=out_specs, check_vma=False
    )
```
